32 devices in a mesh: parts: 2 (over x), rows: 16 (over z, y, core).
Axes of the slice: x: 2, y: 2, z: 4, core: 2. Of those that a mesh axis runs over, the one named last changes fastest.
Arguments:
- pair: bfloat16 [64, 32, 128], P(('parts', 'rows')), parts along dimension 0, may hold values from -16 to 16
- mask: int32 [64], P('parts'), parts along dimension 0, may hold values from 0 to 1, as said below
- w_tri_in: bfloat16 [128, 512], replicated, may hold values from -0.5 to 0.5
- w_tri_gate: bfloat16 [128, 128], replicated, may hold values from -0.5 to 0.5
- w_tri_out: bfloat16 [128, 128], replicated, may hold values from -0.5 to 0.5
- w_qkv: bfloat16 [128, 384], replicated, may hold values from -0.5 to 0.5
- w_att_bias: bfloat16 [128, 4], replicated, may hold values from -80 to 80
- w_att_gate: bfloat16 [128, 128], replicated, may hold values from -0.5 to 0.5
- w_att_out: bfloat16 [128, 128], replicated, may hold values from -0.5 to 0.5
Outputs:
- updated: bfloat16 [64, 32, 128], P(('parts', 'rows')), parts along dimension 0
The draws below stay inside these ranges and needn't reach their ends.
There are 2 independent parts, one for each index of `parts`. The reference program is written for one: setup_inputs(seed, part) draws one part's arguments, and reference() takes and returns one part's arrays. A program takes and returns all parts, laid end to end along the dimension named above; an argument that names none is the same for every part. Nothing has to cross between parts.
Inputs may be any that keep to these rules, and one draw needn't show every extreme that they name: `mask`: 0 on every residue from some L on, with 16 <= L <= 31; before L each residue may be 1 or 0 (unresolved); residue 0 is always 1.
All inputs are finite; a program needn't handle non-finite values.
Results may differ from the reference program's by a relative error of at most 0.012.
Values may be sent and summed in bfloat16 or wider, within the bound.
A program may use at most 64 MiB of HBM per device.

```python
import jax
import jax.numpy as jnp
from jax import lax

CZ = 128
CH = 128
HEADS = 4
HEAD_DIM = 32
ROWS_DEV = 2
RES = 32


def draw_pair(key, part):
    base = jax.random.normal(jax.random.fold_in(key, 11), (RES, RES, CZ), jnp.float32)
    return jnp.clip(base, -16.0, 16.0).astype(jnp.bfloat16)


def draw_mask(key, part):
    length = jax.random.randint(jax.random.fold_in(key, 21), (), RES // 2, RES)
    resolved = jax.random.randint(jax.random.fold_in(key, 22), (RES,), 0, 8) != 0
    positions = jnp.arange(RES)
    keep = (positions < length) & (resolved | (positions == 0))
    return keep.astype(jnp.int32)


def draw_w_att_bias(key, part):
    base = jax.random.normal(jax.random.fold_in(key, 31), (CZ, HEADS), jnp.float32) * CZ ** (-0.5)
    return jnp.clip(base, -80.0, 80.0).astype(jnp.bfloat16)


def bell_draw(rng, shape, scale, most, held_as=jnp.bfloat16):
    values = scale * jax.random.normal(rng, shape, jnp.float32)
    return jnp.clip(values, min=-most, max=most).astype(held_as)


def setup_inputs(seed: int = 0, part: int = 0) -> dict:
    splits = jax.random.split(jax.random.key(seed), 10)
    part_keys = jax.random.split(jax.random.fold_in(splits[9], part), 10)
    return {
        "pair": draw_pair(jax.random.fold_in(jax.random.fold_in(splits[9], part), 71), part),
        "mask": draw_mask(jax.random.fold_in(jax.random.fold_in(splits[9], part), 71), part),
        "w_tri_in": bell_draw(splits[2], (CZ, 4 * CH), CZ ** -0.5, 0.5),
        "w_tri_gate": bell_draw(splits[3], (CZ, CZ), CZ ** -0.5, 0.5),
        "w_tri_out": bell_draw(splits[4], (CH, CZ), CH ** -0.5, 0.5),
        "w_qkv": bell_draw(splits[5], (CZ, 3 * HEADS * HEAD_DIM), CZ ** -0.5, 0.5),
        "w_att_bias": draw_w_att_bias(jax.random.fold_in(splits[9], 71), part),
        "w_att_gate": bell_draw(splits[7], (CZ, HEADS * HEAD_DIM), CZ ** -0.5, 0.5),
        "w_att_out": bell_draw(splits[8], (HEADS * HEAD_DIM, CZ), (HEADS * HEAD_DIM) ** -0.5, 0.5),
    }


EPSILON = 1e-05
MASK_PENALTY = 1000000000.0

def normalize(values, along_axis):
    values = values.astype(jnp.float32)
    center = lax.optimization_barrier(jnp.mean(values, axis=along_axis, keepdims=True))
    shifted = values - center
    spread = lax.optimization_barrier(jnp.mean(shifted * shifted, axis=along_axis, keepdims=True))
    return shifted * lax.rsqrt(spread + EPSILON)

def rounded(values):
    return lax.optimization_barrier(values.astype(jnp.bfloat16))

def attend(queries, key_rows, values, score_bias, key_penalty, score_scale):
    column_count = queries.shape[1]
    heads_here = queries.shape[2]
    block_size = max(1, 4 // heads_here)

    def reorder(tensor):
        return tensor.reshape(tensor.shape[0], column_count // block_size, block_size, heads_here, -1).transpose(1, 0, 2, 3, 4)

    def one_block(inputs):
        query_part, key_part, value_part = inputs
        scores = jnp.einsum('kbhd,ibhd->bhki', key_part.astype(jnp.float32), query_part.astype(jnp.float32)) * score_scale
        scores = scores + score_bias[None] + key_penalty[None, None, :, None]
        row_peak = lax.optimization_barrier(jnp.max(scores, axis=2, keepdims=True))
        weights = jnp.exp(scores - row_peak)
        weights = rounded(weights / lax.optimization_barrier(jnp.sum(weights, axis=2, keepdims=True)))
        result = jnp.einsum('bhki,kbhd->ibhd', weights.astype(jnp.float32), value_part.astype(jnp.float32))
        return result.astype(jnp.bfloat16)
    outputs = lax.map(one_block, (reorder(queries), reorder(key_rows), reorder(values)))
    return outputs.transpose(1, 0, 2, 3, 4).reshape(queries.shape)

def reference(pair, mask, w_tri_in, w_tri_gate, w_tri_out, w_qkv, w_att_bias, w_att_gate, w_att_out):
    key_mask = mask.astype(jnp.float32)
    key_penalty = (key_mask - 1.0) * MASK_PENALTY
    blocks = RES // ROWS_DEV
    row_masks = key_mask.reshape(blocks, ROWS_DEV)
    pair_blocks = pair.reshape(blocks, ROWS_DEV, RES, CZ)

    def first_section(inputs):
        pair_block, row_mask = inputs
        normed = rounded(normalize(pair_block, 2))
        projected = jnp.einsum('rkc,cf->frk', normed.astype(jnp.float32), w_tri_in.astype(jnp.float32))
        pair_mask = row_mask[:, None] * key_mask[None, :]
        left_side = (jax.nn.sigmoid(projected[:CH]) * projected[CH:2 * CH] * pair_mask).astype(jnp.bfloat16)
        right_side = (jax.nn.sigmoid(projected[2 * CH:3 * CH]) * projected[3 * CH:] * pair_mask).astype(jnp.bfloat16)
        return (left_side, right_side)
    left_blocks, right_blocks = lax.map(first_section, (pair_blocks, row_masks))
    left_full = left_blocks.transpose(1, 0, 2, 3).reshape(CH, RES, RES)
    right_full = right_blocks.transpose(1, 0, 2, 3).reshape(CH, RES, RES)

    def contract(inputs):
        left_piece, right_piece = inputs
        return jnp.dot(left_piece, right_piece.T, preferred_element_type=jnp.float32).astype(jnp.bfloat16)
    product = lax.map(contract, (left_full, right_full))
    product_blocks = product.reshape(CH, blocks, ROWS_DEV, RES).transpose(1, 0, 2, 3)

    def second_section(inputs):
        pair_block, triangle_rows = inputs
        normed = rounded(normalize(pair_block, 2))
        triangle_normed = rounded(normalize(triangle_rows, 0))
        triangle_gate = jax.nn.sigmoid(jnp.einsum('rjc,cd->rjd', normed.astype(jnp.float32), w_tri_gate.astype(jnp.float32)))
        triangle_update = jnp.einsum('crj,cd->rjd', triangle_normed.astype(jnp.float32), w_tri_out.astype(jnp.float32))
        middle = rounded(pair_block.astype(jnp.float32) + triangle_gate * triangle_update)
        attention_input = rounded(normalize(middle, 2))
        bias_rows = jnp.einsum('kic,ch->hki', attention_input.astype(jnp.float32), w_att_bias.astype(jnp.float32))
        projections = jnp.einsum('ijc,cf->ijf', attention_input.astype(jnp.float32), w_qkv.astype(jnp.float32)).astype(jnp.bfloat16)
        return (middle, bias_rows, projections)
    middle_blocks, biases, projection_blocks = lax.map(second_section, (pair_blocks, product_blocks))
    bias_full = biases.transpose(1, 0, 2, 3).reshape(HEADS, RES, RES)
    projections = projection_blocks.reshape(RES, RES, 3, HEADS, HEAD_DIM)
    attended = attend(projections[:, :, 0], projections[:, :, 1], projections[:, :, 2], bias_full, key_penalty, HEAD_DIM ** (-0.5))
    attended_blocks = attended.reshape(blocks, ROWS_DEV, RES, HEADS * HEAD_DIM)

    def third_section(inputs):
        middle, attention_rows = inputs
        attention_input = rounded(normalize(middle, 2))
        attention_gate = jax.nn.sigmoid(jnp.einsum('rjc,cf->rjf', attention_input.astype(jnp.float32), w_att_gate.astype(jnp.float32)))
        gated_output = rounded(attention_gate * attention_rows.astype(jnp.float32))
        result = middle.astype(jnp.float32) + jnp.einsum('rjf,fc->rjc', gated_output.astype(jnp.float32), w_att_out.astype(jnp.float32))
        return result.astype(jnp.bfloat16)
    outputs = lax.map(third_section, (middle_blocks, attended_blocks))
    return outputs.reshape(RES, RES, CZ)
```

```python
import functools

import jax
import jax.numpy as jnp
from jax import lax
from jax.experimental import pallas as pl
from jax.experimental.pallas import tpu as pltpu
from jax.sharding import PartitionSpec as P

HEADS = 4
HEAD_DIM = 32
EPSILON = 1e-05
MASK_PENALTY = 1000000000.0
FAR = -1e30
MESH = pl.DeviceIdType.MESH
F32 = jnp.float32
BF16 = jnp.bfloat16
UNROLL = 4


def layer_norm(values):
    center = jnp.mean(values, axis=-1, keepdims=True)
    shifted = values - center
    spread = jnp.mean(shifted * shifted, axis=-1, keepdims=True)
    return shifted * lax.rsqrt(spread + EPSILON)


def dot(a, b):
    return lax.dot_general(a, b, (((1,), (0,)), ((), ())), preferred_element_type=F32)


def dot_nt(a, b):
    return lax.dot_general(a, b, (((1,), (1,)), ((), ())), preferred_element_type=F32)


def repeat(count, body):
    if count <= UNROLL:
        for step in range(count):
            body(step)
    else:
        lax.fori_loop(0, count, lambda step, carry: (body(step), carry)[1], 0)


def iota(shape, axis):
    return lax.broadcasted_iota(jnp.int32, shape, axis)


def kernel(
    n,
    pair_hbm, mask_ref, tri_in_hbm, tri_gate_hbm, tri_out_hbm, qkv_hbm, bias_hbm, gate_hbm, out_hbm,
    result_ref,
    pair_ref, tri_in, tri_gate, tri_out, qkv, att_bias, att_gate, att_out,
    right_buf, input_buf, product, attended,
    load_sem, send_sem, recv_sem,
):
    rows, residues, channels = pair_ref.shape
    total = rows * residues
    chips = n // 2
    me = lax.axis_index("rows")
    chip, core = me // 2, lax.rem(me, 2)
    partner = chip * 2 + (1 - core)

    def peer(offset):
        return lax.rem(chip + offset, chips) * 2 + core

    loads = [
        pltpu.make_async_copy(source, target, load_sem.at[k])
        for k, (source, target) in enumerate(
            [
                (pair_hbm, pair_ref), (tri_in_hbm, tri_in), (tri_gate_hbm, tri_gate),
                (tri_out_hbm, tri_out), (qkv_hbm, qkv), (bias_hbm, att_bias),
                (gate_hbm, att_gate), (out_hbm, att_out),
            ]
        )
    ]
    for load in loads:
        load.start()

    barrier = pltpu.get_barrier_semaphore()

    def greet(device):
        pl.semaphore_signal(barrier, inc=1, device_id={"rows": device}, device_id_type=MESH)

    greet(partner)
    for offset in range(1, chips):
        greet(peer(offset))

    def transfer(buf, which, source, device, slot):
        return pltpu.make_async_remote_copy(
            src_ref=buf.at[source],
            dst_ref=buf.at[source],
            send_sem=send_sem.at[which, slot],
            recv_sem=recv_sem.at[which, source],
            device_id={"rows": device},
            device_id_type=MESH,
        )

    def send_own(buf, which):
        for offset in range(1, chips):
            transfer(buf, which, me, peer(offset), offset).start()
        transfer(buf, which, me, partner, 0).start()

    def forward(buf, which):
        for offset in range(1, chips):
            source = peer(offset)
            transfer(buf, which, source, partner, 0).wait_recv()
            transfer(buf, which, source, partner, chips + offset).start()
        transfer(buf, which, partner, partner, 0).wait_recv()
        for offset in range(1, chips):
            source = lax.rem(chip + offset, chips) * 2 + (1 - core)
            transfer(buf, which, source, partner, 0).wait_recv()

    def finish(buf, which):
        transfer(buf, which, me, partner, 0).wait_send()
        for offset in range(1, chips):
            transfer(buf, which, me, partner, offset).wait_send()
            transfer(buf, which, me, partner, chips + offset).wait_send()

    loads[0].wait()
    first_row = me * rows
    pair = pair_ref[...].reshape(total, channels).astype(F32)
    normed = layer_norm(pair).astype(BF16)
    mask_row = mask_ref[...].astype(F32)
    lane = iota((total, residues), 1)
    line = iota((total, residues), 0)
    key_mask = jnp.sum(jnp.where(lane == line % residues, mask_row, 0.0), axis=1, keepdims=True)
    own_mask = jnp.sum(
        jnp.where(lane == line // residues + first_row, mask_row, 0.0), axis=1, keepdims=True
    )
    pair_mask = key_mask * own_mask
    loads[1].wait()

    def edge(side):
        start = side * 2 * channels
        both = dot(normed, tri_in[:, start : start + 2 * channels])
        return (jax.nn.sigmoid(both[:, :channels]) * both[:, channels:] * pair_mask).astype(BF16)

    right_buf[me] = edge(1).reshape(rows, residues, channels)
    pl.semaphore_wait(barrier, chips)
    send_own(right_buf, 0)
    left = edge(0).astype(F32).reshape(rows, residues, channels)
    loads[2].wait()
    triangle_gate = jax.nn.sigmoid(dot(normed, tri_gate[...]))
    for load in loads[3:]:
        load.wait()

    spread_rows = HEADS * 8
    head_pick = (iota((spread_rows, HEADS), 0) // 8 == iota((spread_rows, HEADS), 1)).astype(BF16)
    bias_rows = dot_nt(head_pick, att_bias[...]).astype(BF16)
    keys = residues * 8
    key_line = iota((residues, keys), 1) // 8 == iota((residues, keys), 0)
    penalty = jnp.sum(
        jnp.where(key_line, (key_mask[:residues] - 1.0) * MASK_PENALTY, 0.0), axis=0, keepdims=True
    )
    same_column = (iota((spread_rows, keys), 0) % 8) == (iota((spread_rows, keys), 1) % 8)
    penalty = jnp.where(same_column, penalty, FAR)

    forward(right_buf, 0)
    group = 8 // rows

    def contract(step):
        start = step * group
        block = right_buf[pl.ds(start, group)].astype(F32).reshape(8, residues, channels)
        at = step * 8 if isinstance(step, int) else pl.multiple_of(step * 8, 8)
        for i in range(rows):
            product[i, pl.ds(at, 8), :] = jnp.sum(block * left[i][None], axis=1)

    repeat(n // group, contract)
    triangle = product[...].reshape(total, channels).astype(BF16).astype(F32)
    triangle_normed = layer_norm(triangle).astype(BF16)
    update = dot(triangle_normed, tri_out[...])
    middle = (pair + triangle_gate * update).astype(BF16).astype(F32)
    attention_input = layer_norm(middle).astype(BF16)
    input_buf[me] = attention_input.reshape(rows, residues, channels)
    send_own(input_buf, 1)

    inner = HEADS * HEAD_DIM
    attention_gate = jax.nn.sigmoid(dot(attention_input, att_gate[...]))
    query = dot(attention_input, qkv[:, :inner]).astype(BF16).astype(F32)
    attended[...] = query.reshape(rows, residues, inner)
    head_of_lane = iota((8, inner), 1) // HEAD_DIM
    finish(right_buf, 0)
    forward(input_buf, 1)

    slab_start = pl.multiple_of(first_row // 16 * 16, 16)
    slab = input_buf[:, :, pl.ds(slab_start, 16), :].astype(F32).reshape(residues, 16, channels)
    within = iota((residues, 16, channels), 1)
    biases = []
    for i in range(rows):
        column = jnp.sum(
            jnp.where(within == first_row - slab_start + i, slab, 0.0), axis=1, keepdims=True
        )
        column = jnp.broadcast_to(column, (residues, 8, channels)).reshape(keys, channels)
        biases.append(dot_nt(bias_rows, column.astype(BF16)) + penalty)
    bias = jnp.concatenate(biases, axis=0)
    scale = HEAD_DIM ** (-0.5)

    def attend(step):
        at = step * 16 if isinstance(step, int) else pl.multiple_of(step * 16, 16)
        source = input_buf[:, :, pl.ds(at, 16), :].reshape(residues * 16, channels)
        both = dot(source, qkv[:, inner:]).reshape(residues, 16, 2 * inner)
        for half in range(2):
            piece = both[:, half * 8 : half * 8 + 8].reshape(keys, 2 * inner).astype(BF16)
            key, value = piece[:, :inner], piece[:, inner:]
            spot = at + half * 8
            if not isinstance(step, int):
                spot = pl.multiple_of(spot, 8)
            queries = []
            for i in range(rows):
                q = attended[i, pl.ds(spot, 8), :]
                queries += [jnp.where(head_of_lane == h, q, 0.0) for h in range(HEADS)]
            scores = dot_nt(jnp.concatenate(queries, axis=0).astype(BF16), key) * scale + bias
            peak = jnp.max(scores, axis=1, keepdims=True)
            weights = jnp.exp(scores - peak)
            weights = (weights / jnp.sum(weights, axis=1, keepdims=True)).astype(BF16)
            mixed = dot(weights, value)
            for i in range(rows):
                picked = jnp.zeros((8, inner), F32)
                for h in range(HEADS):
                    line = (i * HEADS + h) * 8
                    picked = jnp.where(head_of_lane == h, mixed[line : line + 8], picked)
                attended[i, pl.ds(spot, 8), :] = picked

    repeat(residues // 16, attend)
    heads = attended[...].reshape(total, inner).astype(BF16).astype(F32)
    gated = (attention_gate * heads).astype(BF16)
    final = middle + dot(gated, att_out[...])
    result_ref[...] = final.astype(BF16).reshape(rows, residues, channels)
    finish(input_buf, 1)


def solution(mesh):
    n = mesh.shape["rows"]

    def local(pair, mask, *weights):
        rows, residues, channels = pair.shape
        anywhere = pl.BlockSpec(memory_space=pl.ANY)
        vmem = pl.BlockSpec(memory_space=pltpu.VMEM)
        return pl.pallas_call(
            functools.partial(kernel, n),
            out_shape=jax.ShapeDtypeStruct(pair.shape, BF16),
            in_specs=[anywhere, vmem] + [anywhere] * len(weights),
            out_specs=vmem,
            scratch_shapes=[pltpu.VMEM(pair.shape, BF16)]
            + [pltpu.VMEM(w.shape, BF16) for w in weights]
            + [
                pltpu.VMEM((n,) + pair.shape, BF16),
                pltpu.VMEM((n,) + pair.shape, BF16),
                pltpu.VMEM(pair.shape, F32),
                pltpu.VMEM(pair.shape, F32),
                pltpu.SemaphoreType.DMA((1 + len(weights),)),
                pltpu.SemaphoreType.DMA((2, n)),
                pltpu.SemaphoreType.DMA((2, n)),
            ],
            compiler_params=pltpu.CompilerParams(
                collective_id=0, has_side_effects=True, vmem_limit_bytes=62 * 1024 * 1024
            ),
        )(pair, mask.reshape(1, -1), *weights)

    placed = (P(("parts", "rows"), None, None), P("parts")) + (P(),) * 7
    return jax.shard_map(
        local,
        mesh=mesh,
        in_specs=placed,
        out_specs=P(("parts", "rows"), None, None),
        check_vma=False,
    )
```

```python
import functools

import jax
import jax.numpy as jnp
from jax import lax
from jax.experimental import pallas as pl
from jax.experimental.pallas import tpu as pltpu
from jax.sharding import PartitionSpec as P

HEADS = 4
HEAD_DIM = 32
EPSILON = 1e-05
MASK_PENALTY = 1000000000.0
FAR = -1e30
MESH = pl.DeviceIdType.MESH
F32 = jnp.float32
BF16 = jnp.bfloat16
UNROLL = 4


def layer_norm(values):
    center = jnp.mean(values, axis=-1, keepdims=True)
    shifted = values - center
    spread = jnp.mean(shifted * shifted, axis=-1, keepdims=True)
    return shifted * lax.rsqrt(spread + EPSILON)


def dot(a, b):
    return lax.dot_general(a, b, (((1,), (0,)), ((), ())), preferred_element_type=F32)


def dot_nt(a, b):
    return lax.dot_general(a, b, (((1,), (1,)), ((), ())), preferred_element_type=F32)


def repeat(count, body):
    if count <= UNROLL:
        for step in range(count):
            body(step)
    else:
        lax.fori_loop(0, count, lambda step, carry: (body(step), carry)[1], 0)


def split(n):
    chips = n // 2
    minor = 1 << ((chips.bit_length() - 1) // 2)
    return chips, minor, chips // minor


def iota(shape, axis):
    return lax.broadcasted_iota(jnp.int32, shape, axis)


def kernel(
    n,
    pair_hbm, mask_ref, tri_in_hbm, tri_gate_hbm, tri_out_hbm, qkv_hbm, bias_hbm, gate_hbm, out_hbm,
    result_ref,
    pair_ref, tri_in, tri_gate, tri_out, qkv, att_bias, att_gate, att_out,
    right_buf, input_buf, product, attended, queries,
    load_sem, send_sem, recv_sem,
):
    rows, residues, channels = pair_ref.shape
    total = rows * residues
    me = lax.axis_index("rows")
    chips, minor, major = split(n)
    chip, core = me // 2, lax.rem(me, 2)
    place, spot_minor = chip // minor, lax.rem(chip, minor)
    partner = chip * 2 + (1 - core)

    def at_place(a, b, c):
        return (a * minor + b) * 2 + c

    def far(k):
        up = k + (k - place + major) // major
        down_raw = major - 1 - k
        down = down_raw - (place - down_raw + major) // major
        high = place // ((major + 1) // 2)
        return high * up + (1 - high) * down

    majors = [far(k) for k in range(major - 1)]
    minors = [lax.rem(spot_minor + o, minor) for o in range(1, minor)]

    loads = [
        pltpu.make_async_copy(source, target, load_sem.at[k])
        for k, (source, target) in enumerate(
            [
                (pair_hbm, pair_ref), (tri_in_hbm, tri_in), (tri_gate_hbm, tri_gate),
                (tri_out_hbm, tri_out), (qkv_hbm, qkv), (bias_hbm, att_bias),
                (gate_hbm, att_gate), (out_hbm, att_out),
            ]
        )
    ]
    for load in loads:
        load.start()

    barrier = pltpu.get_barrier_semaphore()

    def greet(device):
        pl.semaphore_signal(barrier, inc=1, device_id={"rows": device}, device_id_type=MESH)

    greet(partner)
    for a in majors:
        greet(at_place(a, spot_minor, core))
    for b in minors:
        greet(at_place(place, b, core))
    for a in majors:
        for b in minors:
            greet(at_place(a, b, core))

    def transfer(buf, which, source, device, slot):
        return pltpu.make_async_remote_copy(
            src_ref=buf.at[source],
            dst_ref=buf.at[source],
            send_sem=send_sem.at[which, slot],
            recv_sem=recv_sem.at[which, source],
            device_id={"rows": device},
            device_id_type=MESH,
        )

    def arrived(buf, which, source):
        transfer(buf, which, source, partner, 0).wait_recv()

    def send_own(buf, which):
        slot = 1
        for a in majors:
            for b in minors + [spot_minor]:
                transfer(buf, which, me, at_place(a, b, core), slot).start()
                slot += 1
        for b in minors:
            transfer(buf, which, me, at_place(place, b, core), slot).start()
            slot += 1
        transfer(buf, which, me, partner, 0).start()

    def forward(buf, which):
        slot = chips
        def to_partner(source):
            nonlocal slot
            transfer(buf, which, source, partner, slot).start()
            slot += 1
        for b in minors:
            source = at_place(place, b, core)
            arrived(buf, which, source)
            to_partner(source)
        for a in reversed(majors):
            for b in [spot_minor] + minors:
                source = at_place(a, b, core)
                arrived(buf, which, source)
                to_partner(source)
        arrived(buf, which, partner)
        for b in minors:
            arrived(buf, which, at_place(place, b, 1 - core))
        for a in reversed(majors):
            for b in [spot_minor] + minors:
                arrived(buf, which, at_place(a, b, 1 - core))

    def finish(buf, which):
        for slot in range(2 * chips - 1):
            transfer(buf, which, me, partner, slot).wait_send()

    loads[0].wait()
    first_row = me * rows
    pair = pair_ref[...].reshape(total, channels).astype(F32)
    normed = layer_norm(pair).astype(BF16)
    mask_row = mask_ref[...].astype(F32)
    lane = iota((total, residues), 1)
    line = iota((total, residues), 0)
    key_mask = jnp.sum(jnp.where(lane == line % residues, mask_row, 0.0), axis=1, keepdims=True)
    own_mask = jnp.sum(
        jnp.where(lane == line // residues + first_row, mask_row, 0.0), axis=1, keepdims=True
    )
    pair_mask = key_mask * own_mask
    loads[1].wait()

    def edge(side):
        start = side * 2 * channels
        both = dot(normed, tri_in[:, start : start + 2 * channels])
        return (jax.nn.sigmoid(both[:, :channels]) * both[:, channels:] * pair_mask).astype(BF16)

    right_buf[me] = edge(1).reshape(rows, residues, channels)
    pl.semaphore_wait(barrier, chips)
    send_own(right_buf, 0)
    left = edge(0).astype(F32).reshape(rows, residues, channels)
    loads[2].wait()
    triangle_gate = jax.nn.sigmoid(dot(normed, tri_gate[...]))
    for load in loads[3:]:
        load.wait()

    width = 16
    spread_rows = HEADS * width
    head_pick = (iota((spread_rows, HEADS), 0) // width == iota((spread_rows, HEADS), 1)).astype(BF16)
    bias_rows = dot(head_pick, att_bias[...]).astype(BF16)
    keys = residues * width
    key_line = iota((residues, keys), 1) // width == iota((residues, keys), 0)
    penalty = jnp.sum(
        jnp.where(key_line, (key_mask[:residues] - 1.0) * MASK_PENALTY, 0.0), axis=0, keepdims=True
    )
    same_column = (iota((spread_rows, keys), 0) % width) == (iota((spread_rows, keys), 1) % width)
    penalty = jnp.where(same_column, penalty, FAR)

    forward(right_buf, 0)
    group = 8 // rows

    def contract(step):
        start = step * group
        block = right_buf[pl.ds(start, group)].astype(F32).reshape(8, residues, channels)
        at = step * 8 if isinstance(step, int) else pl.multiple_of(step * 8, 8)
        for i in range(rows):
            product[i, pl.ds(at, 8), :] = jnp.sum(block * left[i][None], axis=1)

    repeat(n // group, contract)
    triangle = product[...].reshape(total, channels).astype(BF16).astype(F32)
    triangle_normed = layer_norm(triangle).astype(BF16)
    update = dot(triangle_normed, tri_out[...])
    middle = (pair + triangle_gate * update).astype(BF16).astype(F32)
    attention_input = layer_norm(middle).astype(BF16)
    input_buf[me] = attention_input.reshape(rows, residues, channels)
    send_own(input_buf, 1)

    inner = HEADS * HEAD_DIM
    attention_gate = jax.nn.sigmoid(dot(attention_input, att_gate[...]))
    query = dot(attention_input, qkv[:, :inner]).astype(BF16).astype(F32)
    query = query.reshape(rows, residues, inner)
    head_of_lane = iota((width, inner), 1) // HEAD_DIM
    scale = HEAD_DIM ** (-0.5)
    per_block = rows * spread_rows
    for block in range(residues // width):
        parts = []
        for i in range(rows):
            q = query[i, block * width : (block + 1) * width]
            parts += [jnp.where(head_of_lane == h, q, 0.0) for h in range(HEADS)]
        turned = dot_nt(jnp.concatenate(parts, axis=0).astype(BF16), qkv[:, inner : 2 * inner])
        queries[block] = (turned * scale).astype(BF16)
    finish(right_buf, 0)
    forward(input_buf, 1)

    slab_start = pl.multiple_of(first_row // width * width, width)
    slab = input_buf[:, :, pl.ds(slab_start, width), :].astype(F32).reshape(residues, width, channels)
    within = iota((residues, width, channels), 1)
    biases = []
    for i in range(rows):
        column = jnp.sum(
            jnp.where(within == first_row - slab_start + i, slab, 0.0), axis=1, keepdims=True
        )
        column = jnp.broadcast_to(column, (residues, width, channels)).reshape(keys, channels)
        biases.append(dot_nt(bias_rows, column.astype(BF16)) + penalty)
    bias = jnp.concatenate(biases, axis=0)

    def attend(step):
        at = step * width if isinstance(step, int) else pl.multiple_of(step * width, width)
        source = input_buf[:, :, pl.ds(at, width), :].reshape(keys, channels)
        scores = dot_nt(queries[step], source) + bias
        peak = jnp.max(scores, axis=1, keepdims=True)
        weights = jnp.exp(scores - peak)
        whole = jnp.sum(weights, axis=1, keepdims=True)
        mixed = dot(weights.astype(BF16), source) / whole
        valued = dot(mixed.astype(BF16), qkv[:, 2 * inner :])
        for i in range(rows):
            picked = jnp.zeros((width, inner), F32)
            for h in range(HEADS):
                line = (i * HEADS + h) * width
                picked = jnp.where(head_of_lane == h, valued[line : line + width], picked)
            attended[i, pl.ds(at, width), :] = picked

    repeat(residues // width, attend)
    heads = attended[...].reshape(total, inner).astype(BF16).astype(F32)
    gated = (attention_gate * heads).astype(BF16)
    final = middle + dot(gated, att_out[...])
    result_ref[...] = final.astype(BF16).reshape(rows, residues, channels)
    finish(input_buf, 1)


def solution(mesh):
    n = mesh.shape["rows"]

    def local(pair, mask, *weights):
        weights = weights[:4] + (weights[4].T,) + weights[5:]
        rows, residues, channels = pair.shape
        anywhere = pl.BlockSpec(memory_space=pl.ANY)
        vmem = pl.BlockSpec(memory_space=pltpu.VMEM)
        return pl.pallas_call(
            functools.partial(kernel, n),
            out_shape=jax.ShapeDtypeStruct(pair.shape, BF16),
            in_specs=[anywhere, vmem] + [anywhere] * len(weights),
            out_specs=vmem,
            scratch_shapes=[pltpu.VMEM(pair.shape, BF16)]
            + [pltpu.VMEM(w.shape, BF16) for w in weights]
            + [
                pltpu.VMEM((n,) + pair.shape, BF16),
                pltpu.VMEM((n,) + pair.shape, BF16),
                pltpu.VMEM(pair.shape, F32),
                pltpu.VMEM(pair.shape, F32),
                pltpu.VMEM((residues // 16, rows * HEADS * 16, HEADS * HEAD_DIM), BF16),
                pltpu.SemaphoreType.DMA((1 + len(weights),)),
                pltpu.SemaphoreType.DMA((2, n)),
                pltpu.SemaphoreType.DMA((2, n)),
            ],
            compiler_params=pltpu.CompilerParams(
                collective_id=0, has_side_effects=True, vmem_limit_bytes=62 << 20
            ),
        )(pair, mask.reshape(1, -1), *weights)

    placed = (P(("parts", "rows"), None, None), P("parts")) + (P(),) * 7
    return jax.shard_map(
        local,
        mesh=mesh,
        in_specs=placed,
        out_specs=P(("parts", "rows"), None, None),
        check_vma=False,
    )
```

```python
import functools

import jax
import jax.numpy as jnp
from jax import lax
from jax.experimental import pallas as pl
from jax.experimental.pallas import tpu as pltpu
from jax.sharding import PartitionSpec as P

HEADS = 4
HEAD_DIM = 32
EPSILON = 1e-05
MASK_PENALTY = 1000000000.0
FAR = -1e30
MESH = pl.DeviceIdType.MESH
F32 = jnp.float32
BF16 = jnp.bfloat16
UNROLL = 4
VMEM_LIMIT = int(53.905 * 2**20)


def layer_norm(values):
    center = jnp.mean(values, axis=-1, keepdims=True)
    shifted = values - center
    spread = jnp.mean(shifted * shifted, axis=-1, keepdims=True)
    return shifted * lax.rsqrt(spread + EPSILON)


def dot(a, b):
    return lax.dot_general(a, b, (((1,), (0,)), ((), ())), preferred_element_type=F32)


def dot_nt(a, b):
    return lax.dot_general(a, b, (((1,), (1,)), ((), ())), preferred_element_type=F32)


def repeat(count, body):
    if count <= UNROLL:
        for step in range(count):
            body(step)
    else:
        lax.fori_loop(0, count, lambda step, carry: (body(step), carry)[1], 0)


def split(n):
    chips = n // 2
    minor = 1 << ((chips.bit_length() - 1) // 2)
    return chips, minor, chips // minor


def iota(shape, axis):
    return lax.broadcasted_iota(jnp.int32, shape, axis)


def kernel(
    n,
    pair_hbm, mask_ref, tri_in_hbm, tri_gate_hbm, tri_out_hbm, qkv_hbm, bias_hbm, gate_hbm, out_hbm,
    result_ref,
    pair_ref, tri_in, tri_gate, tri_out, qkv, att_bias, att_gate, att_out,
    right_buf, input_buf, product, attended, queries,
    load_sem, send_sem, recv_sem,
):
    rows, residues, channels = pair_ref.shape
    total = rows * residues
    me = lax.axis_index("rows")
    chips, minor, major = split(n)
    chip, core = me // 2, lax.rem(me, 2)
    place, spot_minor = chip // minor, lax.rem(chip, minor)
    partner = chip * 2 + (1 - core)

    def at_place(a, b, c):
        return (a * minor + b) * 2 + c

    def far(k):
        up = k + (k - place + major) // major
        down_raw = major - 1 - k
        down = down_raw - (place - down_raw + major) // major
        high = place // ((major + 1) // 2)
        return high * up + (1 - high) * down

    majors = [far(k) for k in range(major - 1)]
    minors = [lax.rem(spot_minor + o, minor) for o in range(1, minor)]

    loads = [
        pltpu.make_async_copy(source, target, load_sem.at[k])
        for k, (source, target) in enumerate(
            [
                (pair_hbm, pair_ref), (tri_in_hbm, tri_in), (tri_gate_hbm, tri_gate),
                (tri_out_hbm, tri_out), (qkv_hbm, qkv), (bias_hbm, att_bias),
                (gate_hbm, att_gate), (out_hbm, att_out),
            ]
        )
    ]
    loads[0].start()

    barrier = pltpu.get_barrier_semaphore()

    def greet(device):
        pl.semaphore_signal(barrier, inc=1, device_id={"rows": device}, device_id_type=MESH)

    greet(partner)
    for a in majors:
        greet(at_place(a, spot_minor, core))
    for b in minors:
        greet(at_place(place, b, core))
    for a in majors:
        for b in minors:
            greet(at_place(a, b, core))

    for load in loads[1:]:
        load.start()

    def transfer(buf, which, source, device, slot):
        return pltpu.make_async_remote_copy(
            src_ref=buf.at[source],
            dst_ref=buf.at[source],
            send_sem=send_sem.at[which, slot],
            recv_sem=recv_sem.at[which, source],
            device_id={"rows": device},
            device_id_type=MESH,
        )

    def arrived(buf, which, source):
        transfer(buf, which, source, partner, 0).wait_recv()

    def send_own(buf, which):
        slot = 1
        pairs = [(a, b) for b in minors for a in majors] + [(a, spot_minor) for a in majors]
        for a, b in pairs:
            transfer(buf, which, me, at_place(a, b, core), slot).start()
            slot += 1
        for b in minors:
            transfer(buf, which, me, at_place(place, b, core), slot).start()
            slot += 1
        transfer(buf, which, me, partner, 0).start()

    def forward(buf, which):
        slot = chips
        def to_partner(source):
            nonlocal slot
            transfer(buf, which, source, partner, slot).start()
            slot += 1
        for b in minors:
            source = at_place(place, b, core)
            arrived(buf, which, source)
            to_partner(source)
        for a in reversed(majors):
            for b in [spot_minor] + minors:
                source = at_place(a, b, core)
                arrived(buf, which, source)
                to_partner(source)
        arrived(buf, which, partner)
        for b in minors:
            arrived(buf, which, at_place(place, b, 1 - core))
        for a in reversed(majors):
            for b in [spot_minor] + minors:
                arrived(buf, which, at_place(a, b, 1 - core))

    def finish(buf, which):
        for slot in range(2 * chips - 1):
            transfer(buf, which, me, partner, slot).wait_send()

    loads[0].wait()
    first_row = me * rows
    pair = pair_ref[...].reshape(total, channels).astype(F32)
    normed = layer_norm(pair).astype(BF16)
    mask_row = mask_ref[...].astype(F32)
    lane = iota((total, residues), 1)
    line = iota((total, residues), 0)
    key_mask = jnp.sum(jnp.where(lane == line % residues, mask_row, 0.0), axis=1, keepdims=True)
    own_mask = jnp.sum(
        jnp.where(lane == line // residues + first_row, mask_row, 0.0), axis=1, keepdims=True
    )
    pair_mask = key_mask * own_mask
    loads[1].wait()

    def edge(side):
        start = side * 2 * channels
        both = dot(normed, tri_in[:, start : start + 2 * channels])
        return (jax.nn.sigmoid(both[:, :channels]) * both[:, channels:] * pair_mask).astype(BF16)

    right_buf[me] = edge(1).reshape(rows, residues, channels)
    pl.semaphore_wait(barrier, chips)
    send_own(right_buf, 0)
    left = edge(0).astype(F32).reshape(rows, residues, channels)
    loads[2].wait()
    triangle_gate = jax.nn.sigmoid(dot(normed, tri_gate[...]))
    for load in loads[3:]:
        load.wait()

    width = 16
    spread_rows = HEADS * width
    head_pick = (iota((spread_rows, HEADS), 0) // width == iota((spread_rows, HEADS), 1)).astype(BF16)
    bias_rows = dot(head_pick, att_bias[...]).astype(BF16)
    keys = residues * width
    key_line = iota((residues, keys), 1) // width == iota((residues, keys), 0)
    penalty = jnp.sum(
        jnp.where(key_line, (key_mask[:residues] - 1.0) * MASK_PENALTY, 0.0), axis=0, keepdims=True
    )
    same_column = (iota((spread_rows, keys), 0) % width) == (iota((spread_rows, keys), 1) % width)
    penalty = jnp.where(same_column, penalty, FAR)

    forward(right_buf, 0)
    group = 8 // rows

    def contract(step):
        start = step * group
        block = right_buf[pl.ds(start, group)].astype(F32).reshape(8, residues, channels)
        at = step * 8 if isinstance(step, int) else pl.multiple_of(step * 8, 8)
        for i in range(rows):
            product[i, pl.ds(at, 8), :] = jnp.sum(block * left[i][None], axis=1)

    repeat(n // group, contract)
    triangle = product[...].reshape(total, channels).astype(BF16).astype(F32)
    triangle_normed = layer_norm(triangle).astype(BF16)
    update = dot(triangle_normed, tri_out[...])
    middle = (pair + triangle_gate * update).astype(BF16).astype(F32)
    attention_input = layer_norm(middle).astype(BF16)
    input_buf[me] = attention_input.reshape(rows, residues, channels)
    send_own(input_buf, 1)

    inner = HEADS * HEAD_DIM
    attention_gate = jax.nn.sigmoid(dot(attention_input, att_gate[...]))
    query = dot(attention_input, qkv[:, :inner]).astype(BF16).astype(F32)
    query = query.reshape(rows, residues, inner)
    head_of_lane = iota((width, inner), 1) // HEAD_DIM
    scale = HEAD_DIM ** (-0.5)
    per_block = rows * spread_rows
    for block in range(residues // width):
        parts = []
        for i in range(rows):
            q = query[i, block * width : (block + 1) * width]
            parts += [jnp.where(head_of_lane == h, q, 0.0) for h in range(HEADS)]
        turned = dot_nt(jnp.concatenate(parts, axis=0).astype(BF16), qkv[:, inner : 2 * inner])
        queries[block] = (turned * scale).astype(BF16)
    finish(right_buf, 0)
    forward(input_buf, 1)

    slab_start = pl.multiple_of(first_row // width * width, width)
    slab = input_buf[:, :, pl.ds(slab_start, width), :].astype(F32).reshape(residues, width, channels)
    within = iota((residues, width, channels), 1)
    biases = []
    for i in range(rows):
        column = jnp.sum(
            jnp.where(within == first_row - slab_start + i, slab, 0.0), axis=1, keepdims=True
        )
        column = jnp.broadcast_to(column, (residues, width, channels)).reshape(keys, channels)
        biases.append(dot_nt(bias_rows, column.astype(BF16)) + penalty)
    bias = jnp.concatenate(biases, axis=0)

    def attend(step):
        at = step * width if isinstance(step, int) else pl.multiple_of(step * width, width)
        source = input_buf[:, :, pl.ds(at, width), :].reshape(keys, channels)
        scores = dot_nt(queries[step], source) + bias
        peak = jnp.max(scores, axis=1, keepdims=True)
        weights = jnp.exp(scores - peak)
        whole = jnp.sum(weights, axis=1, keepdims=True)
        mixed = dot(weights.astype(BF16), source) / whole
        valued = dot(mixed.astype(BF16), qkv[:, 2 * inner :])
        for i in range(rows):
            picked = jnp.zeros((width, inner), F32)
            for h in range(HEADS):
                line = (i * HEADS + h) * width
                picked = jnp.where(head_of_lane == h, valued[line : line + width], picked)
            attended[i, pl.ds(at, width), :] = picked

    repeat(residues // width, attend)
    heads = attended[...].reshape(total, inner).astype(BF16).astype(F32)
    gated = (attention_gate * heads).astype(BF16)
    final = middle + dot(gated, att_out[...])
    result_ref[...] = final.astype(BF16).reshape(rows, residues, channels)
    finish(input_buf, 1)


def solution(mesh):
    n = mesh.shape["rows"]

    def local(pair, mask, *weights):
        weights = weights[:4] + (weights[4].T,) + weights[5:]
        rows, residues, channels = pair.shape
        anywhere = pl.BlockSpec(memory_space=pl.ANY)
        vmem = pl.BlockSpec(memory_space=pltpu.VMEM)
        return pl.pallas_call(
            functools.partial(kernel, n),
            out_shape=jax.ShapeDtypeStruct(pair.shape, BF16),
            in_specs=[anywhere, vmem] + [anywhere] * len(weights),
            out_specs=vmem,
            scratch_shapes=[pltpu.VMEM(pair.shape, BF16)]
            + [pltpu.VMEM(w.shape, BF16) for w in weights]
            + [
                pltpu.VMEM((n,) + pair.shape, BF16),
                pltpu.VMEM((n,) + pair.shape, BF16),
                pltpu.VMEM(pair.shape, F32),
                pltpu.VMEM(pair.shape, F32),
                pltpu.VMEM((residues // 16, rows * HEADS * 16, HEADS * HEAD_DIM), BF16),
                pltpu.SemaphoreType.DMA((1 + len(weights),)),
                pltpu.SemaphoreType.DMA((2, n)),
                pltpu.SemaphoreType.DMA((2, n)),
            ],
            compiler_params=pltpu.CompilerParams(
                collective_id=0, has_side_effects=True, vmem_limit_bytes=VMEM_LIMIT
            ),
        )(pair, mask.reshape(1, -1), *weights)

    placed = (P(("parts", "rows"), None, None), P("parts")) + (P(),) * 7
    return jax.shard_map(
        local,
        mesh=mesh,
        in_specs=placed,
        out_specs=P(("parts", "rows"), None, None),
        check_vma=False,
    )
```
